32 devices in a mesh: seq: 16 (over z, x, core), fsdp: 2 (over y).
Axes of the slice: x: 2, y: 2, z: 4, core: 2. Of those that a mesh axis runs over, the one named last changes fastest.
Arguments:
- queries: bfloat16 [8192, 2048], P(('seq', 'fsdp')), may hold values from -150 to 150
- key_rotated_rows: bfloat16 [8192, 1024], P(('seq', 'fsdp')), may hold values from -5 to 5
- values: bfloat16 [8192, 1024], P(('seq', 'fsdp')), may hold values from -6 to 6
- out_weight: bfloat16 [2048, 5376], P('seq', 'fsdp'), may hold values from -0.125 to 0.125
- residual: bfloat16 [8192, 5376], P(('seq', 'fsdp')), may hold values from -6 to 6
- norm_gain: float32 [5376], replicated, may hold values from 0.25 to 1.75
- doc_lengths: int32 [8], replicated, may hold values from 1 to 2048, 8192 in all
Outputs:
- output: bfloat16 [8192, 5376], P(('seq', 'fsdp'))
The draws below stay inside these ranges and needn't reach their ends.
All inputs are finite; a program needn't handle non-finite values.
Results may differ from the reference program's by a relative error of at most 0.007.
Values may be sent and summed in bfloat16 or wider, within the bound.
No kernel may reach another device: no remote copies, remote signals or barrier semaphores. Data moves between devices by JAX's collectives and lax.ppermute only.
A program may use at most 128 MiB of HBM per device.

```python
import math
import jax
import jax.numpy as jnp
import numpy as np
from jax import lax

D = 5376
QUERY_HEADS = 16
KEY_VALUE_HEADS = 8
HEAD_SIZE = 128
WINDOW_TOKENS = 1024
QSCALE = 168
TOKENS_PER_SHARD = 256
CONTEXT_TOKENS = 8192
DOCS = 8


def draw_pair(key):
    base = jax.random.fold_in(key, 4242)
    first_segment, part_b = jax.random.split(base, 2)
    key_rotated_rows = jnp.clip(jax.random.normal(first_segment, (CONTEXT_TOKENS, KEY_VALUE_HEADS * HEAD_SIZE), jnp.float32), -4.5, 4.5)
    queries = jnp.clip(jax.random.normal(part_b, (CONTEXT_TOKENS, QUERY_HEADS * HEAD_SIZE), jnp.float32), -4.0, 4.0)
    return (queries, key_rotated_rows)


def draw_queries(key, part):
    return draw_pair(key)[0].astype(jnp.bfloat16)


def draw_key_rotated_rows(key, part):
    return draw_pair(key)[1].astype(jnp.bfloat16)


def block_scale(stream_key, shape, shards, low, high):
    level, own = 1.0, jax.random.fold_in(stream_key, 6)
    for position, blocks in shards:
        heights = jnp.exp(jax.random.uniform(jax.random.fold_in(own, position), (blocks,), jnp.float32, low / len(shards), high / len(shards)))
        level = level * jnp.repeat(heights, shape[position] // blocks).reshape([-1 if axis == position else 1 for axis in range(len(shape))])
    return level


def split_up(number_of, total, reach, lean):
    portions = [(1 << 20) // math.isqrt(rank ** lean) + 1 for rank in range(2, number_of + 1)]
    rest, holding = total - reach - (number_of - 1), [1] * (number_of - 1)
    while rest > 0:
        free = [i for i in range(number_of - 1) if holding[i] < reach]
        mass, remaining = sum([portions[i] for i in free]), rest
        for i in free:
            addition = min(reach - holding[i], max(1, remaining * portions[i] // mass), rest)
            holding[i] = holding[i] + addition
            rest = rest - addition
    return np.array([reach] + holding)


def uneven_parts(key, number_of, total, reach, slope):
    if number_of == 2:
        one = jax.random.randint(key, (), max(1, total - reach), min(reach, total - 1) + 1)
        return jnp.stack([one, total - one])
    sizes = jnp.asarray(split_up(number_of, total, reach, slope), jnp.int32)
    pairs = (number_of - 1) // 2
    donor, sink = sizes[1:1 + 2 * pairs:2], sizes[2:2 + 2 * pairs:2]
    slack = jnp.minimum(donor - 1, reach - sink)
    shifted = jax.random.randint(jax.random.fold_in(key, 1), (pairs,), 0, 1 << 20) % (slack + 1)
    sizes = sizes.at[1:1 + 2 * pairs:2].set(donor - shifted).at[2:2 + 2 * pairs:2].set(sink + shifted)
    return sizes[jax.random.permutation(jax.random.fold_in(key, 2), number_of)]


def centred(own_key, dims, deviation, limit, shards=(), kind=jnp.bfloat16):
    array = deviation * jax.random.normal(own_key, dims, jnp.float32)
    if shards:
        array = array * block_scale(own_key, dims, shards, -0.22, 0.18)
    return jnp.clip(array, -limit, limit).astype(kind)


def setup_inputs(seed: int = 0) -> dict:
    keys = jax.random.split(jax.random.key(seed), 8)
    return {
        "queries": draw_queries(jax.random.fold_in(keys[7], 71), 0),
        "key_rotated_rows": draw_key_rotated_rows(jax.random.fold_in(keys[7], 71), 0),
        "values": centred(keys[2], (CONTEXT_TOKENS, KEY_VALUE_HEADS * HEAD_SIZE), 1.0, 6.0, ((0, 32),)),
        "out_weight": centred(keys[3], (QUERY_HEADS * HEAD_SIZE, D), (QUERY_HEADS * HEAD_SIZE) ** -0.5, 0.125, ((0, 16), (1, 2))),
        "residual": centred(keys[4], (CONTEXT_TOKENS, D), 1.0, 6.0, ((0, 32),)),
        "norm_gain": jnp.clip(1.0 + 0.15 * jax.random.normal(keys[5], (D,), jnp.float32), 0.25, 1.75),
        "doc_lengths": uneven_parts(keys[6], DOCS, CONTEXT_TOKENS, 8 * TOKENS_PER_SHARD, 2).astype(jnp.int32),
    }


def doc_index(positions, starts):
    return lax.optimization_barrier(jnp.sum((starts[None, :] <= positions[:, None]).astype(jnp.int32), axis=1)) - 1

def reference(queries, key_rotated_rows, values, out_weight, residual, norm_gain, doc_lengths):
    queries_per_group = QUERY_HEADS // KEY_VALUE_HEADS
    scaling = QSCALE ** (-0.5)
    starts = jnp.cumsum(doc_lengths) - doc_lengths
    key_padded_rows = jnp.concatenate([jnp.zeros((WINDOW_TOKENS, KEY_VALUE_HEADS * HEAD_SIZE), key_rotated_rows.dtype), key_rotated_rows], axis=0)
    value_padded_rows = jnp.concatenate([jnp.zeros((WINDOW_TOKENS, KEY_VALUE_HEADS * HEAD_SIZE), values.dtype), values], axis=0)

    def block(block_index):
        token_offset = (block_index * TOKENS_PER_SHARD).astype(jnp.int32)
        query_block_tile = lax.dynamic_slice_in_dim(queries, token_offset, TOKENS_PER_SHARD, 0).reshape(TOKENS_PER_SHARD, KEY_VALUE_HEADS, queries_per_group, HEAD_SIZE).astype(jnp.float32)
        key_block_tile = lax.dynamic_slice_in_dim(key_padded_rows, token_offset, WINDOW_TOKENS + TOKENS_PER_SHARD, 0).reshape(WINDOW_TOKENS + TOKENS_PER_SHARD, KEY_VALUE_HEADS, HEAD_SIZE).astype(jnp.float32)
        value_block_tile = lax.dynamic_slice_in_dim(value_padded_rows, token_offset, WINDOW_TOKENS + TOKENS_PER_SHARD, 0).reshape(WINDOW_TOKENS + TOKENS_PER_SHARD, KEY_VALUE_HEADS, HEAD_SIZE).astype(jnp.float32)
        q_pos = token_offset + jnp.arange(TOKENS_PER_SHARD, dtype=jnp.int32)
        k_pos = token_offset - WINDOW_TOKENS + jnp.arange(WINDOW_TOKENS + TOKENS_PER_SHARD, dtype=jnp.int32)
        lag = q_pos[:, None] - k_pos[None, :]
        allowed = (doc_index(q_pos, starts)[:, None] == doc_index(k_pos, starts)[None, :]) & (lag >= 0) & (lag < WINDOW_TOKENS) & (k_pos[None, :] >= 0)
        scores = jnp.einsum('qhgd,khd->hgqk', query_block_tile, key_block_tile) * scaling
        scores = jnp.where(allowed[None, None], scores, -jnp.inf)
        peak = lax.optimization_barrier(jnp.max(scores, axis=-1, keepdims=True))
        expon = jnp.exp(scores - peak)
        probs = (expon / lax.optimization_barrier(jnp.sum(expon, axis=-1, keepdims=True))).astype(jnp.bfloat16)
        mixed = jnp.einsum('hgqk,khd->qhgd', probs.astype(jnp.float32), value_block_tile)
        return mixed.reshape(TOKENS_PER_SHARD, QUERY_HEADS * HEAD_SIZE).astype(jnp.bfloat16)
    attended = lax.map(block, jnp.arange(CONTEXT_TOKENS // TOKENS_PER_SHARD, dtype=jnp.int32)).reshape(CONTEXT_TOKENS, QUERY_HEADS * HEAD_SIZE)
    projected = jnp.dot(attended, out_weight, preferred_element_type=jnp.float32)
    meansq = lax.optimization_barrier(jnp.mean(projected * projected, axis=-1, keepdims=True))
    output = residual.astype(jnp.float32) + norm_gain.astype(jnp.float32) * projected * lax.rsqrt(meansq + 1e-06)
    return output.astype(jnp.bfloat16)
```

```python
import functools
import math

import jax
import jax.numpy as jnp
from jax import lax
from jax.experimental import pallas as pl
from jax.experimental.pallas import tpu as pltpu
from jax.sharding import PartitionSpec as P

QUERY_HEADS = 16
KEY_VALUE_HEADS = 8
HEAD_SIZE = 128
WINDOW_TOKENS = 1024
QSCALE = 168
SUB = 128
NEG = -1e30


ANY = pl.BlockSpec(memory_space=pl.ANY)
VM = pl.BlockSpec(memory_space=pltpu.VMEM)
SM = pl.BlockSpec(memory_space=pltpu.SMEM)


def attend_kernel(rows, heads, groups, f_ref, lo_ref, qa, qb, *rest):
    kv = rest[:6]
    out_ref, q_all, kv_all, sems = rest[6:]
    f = f_ref[0]
    copies = []
    for i, (src, at) in enumerate(((qa, f), (qb, 1 - f))):
        copies.append(pltpu.make_async_copy(src, q_all.at[pl.ds(pl.multiple_of(at * rows, rows), rows)], sems.at[i]))
    for i in range(6):
        at = 2 * (i // 2) + (f if i % 2 == 0 else 1 - f)
        copies.append(pltpu.make_async_copy(kv[i], kv_all.at[pl.ds(pl.multiple_of(at * rows, rows), rows)], sems.at[2 + i]))
    for copy in copies:
        copy.start()
    for copy in copies:
        copy.wait()
    span = WINDOW_TOKENS + SUB
    half = heads * HEAD_SIZE
    factor = QSCALE ** (-0.5) * math.log2(math.e)
    column = lax.broadcasted_iota(jnp.int32, (1, span), 1)
    row = lax.broadcasted_iota(jnp.int32, (SUB, 1), 0)

    def step(t, _):
        base = pl.multiple_of(t * SUB, SUB)
        low = lo_ref[pl.ds(base, SUB), :] - base
        allowed = (column >= low) & (column <= row + WINDOW_TOKENS)
        allowed = jnp.concatenate([allowed] * groups, axis=0)
        for g in range(heads):
            q = q_all[pl.ds(base, SUB), g * groups * HEAD_SIZE : (g + 1) * groups * HEAD_SIZE]
            q = jnp.concatenate([q[:, i * HEAD_SIZE : (i + 1) * HEAD_SIZE] for i in range(groups)], axis=0)
            k = kv_all[pl.ds(base, span), g * HEAD_SIZE : (g + 1) * HEAD_SIZE]
            v = kv_all[pl.ds(base, span), half + g * HEAD_SIZE : half + (g + 1) * HEAD_SIZE]
            s = lax.dot_general(q, k, (((1,), (1,)), ((), ())), preferred_element_type=jnp.float32)
            s = jnp.where(allowed, s, -jnp.inf)
            peak = jnp.max(s, axis=1, keepdims=True)
            e = jnp.exp2((s - peak) * factor)
            total = jnp.sum(e, axis=1, keepdims=True)
            o = jnp.dot(e.astype(jnp.bfloat16), v, preferred_element_type=jnp.float32) / total
            for i in range(groups):
                at = (g * groups + i) * HEAD_SIZE
                out_ref[pl.ds(base, SUB), at : at + HEAD_SIZE] = o[i * SUB : (i + 1) * SUB].astype(jnp.bfloat16)
        return 0

    lax.fori_loop(0, 2 * rows // SUB, step, 0)


def project_kernel(rows, pieces, f_ref, at_ref, mine, other, *rest):
    parts = rest[:pieces]
    own_ref, send_ref, weight, sems = rest[pieces:]
    depth = weight.shape[0] // pieces
    f = f_ref[0]
    copies = []
    for i in range(pieces):
        at = pl.multiple_of(at_ref[i] * depth, depth)
        copies.append(pltpu.make_async_copy(parts[i], weight.at[pl.ds(at, depth)], sems.at[i]))
    for copy in copies:
        copy.start()
    for copy in copies:
        copy.wait()
    half = mine.shape[1]
    first = pl.ds(pl.multiple_of(f * half, half), half)
    second = pl.ds(pl.multiple_of((1 - f) * half, half), half)
    width = weight.shape[1]
    tile = 384 if width % 384 == 0 else 128

    def product(at, columns):
        part = jnp.dot(mine[at, :], weight[first, columns], preferred_element_type=jnp.float32)
        return part + jnp.dot(other[at, :], weight[second, columns], preferred_element_type=jnp.float32)

    mine_rows = pl.ds(pl.multiple_of(f * rows, rows), rows)
    other_rows = pl.ds(pl.multiple_of((1 - f) * rows, rows), rows)

    def step(n, _):
        columns = pl.ds(pl.multiple_of(n * tile, tile), tile)
        send_ref[:, columns] = product(other_rows, columns).astype(jnp.bfloat16)
        own_ref[:, columns] = product(mine_rows, columns)
        return 0

    lax.fori_loop(0, width // tile, step, 0)


def finish_kernel(f_ref, own, got, residual, gain, out_ref):
    f = f_ref[0]
    width = own.shape[1]
    total = residual.shape[1]
    a = own[...]
    b = got[...].astype(jnp.float32)
    mean = (jnp.sum(a * a, axis=1, keepdims=True) + jnp.sum(b * b, axis=1, keepdims=True)) / total
    scale = lax.rsqrt(mean + 1e-06)
    for part, at in ((a, f), (b, 1 - f)):
        columns = pl.ds(pl.multiple_of(at * width, 128), width)
        value = residual[:, columns].astype(jnp.float32) + gain[:, columns] * part * scale
        out_ref[:, columns] = value.astype(jnp.bfloat16)


def send(value, axis, pairs):
    return lax.ppermute(value, axis, pairs)


def shards(queries, key_rotated_rows, values, out_weight, residual, norm_gain, doc_lengths):
    rows = queries.shape[0]
    groups = QUERY_HEADS // KEY_VALUE_HEADS
    count = lax.axis_size("seq")
    behind = WINDOW_TOKENS // (2 * rows)
    if lax.axis_size("fsdp") != 2 or behind != 2 or count % 4:
        raise ValueError("unsupported shape")
    heads = KEY_VALUE_HEADS // 2
    s = lax.axis_index("seq")
    f = lax.axis_index("fsdp")
    c = s % 2
    flag = f.astype(jnp.int32).reshape(1)
    swap = [(0, 1), (1, 0)]
    cores = [(i, i ^ 1) for i in range(count)]
    upper = f == 0

    def half_of(x, other):
        width = x.shape[1] // 2
        low, high = x[:, :width], x[:, width:]
        return jnp.where(upper != other, low, high)

    kv_own = jnp.concatenate([half_of(key_rotated_rows, False), half_of(values, False)], axis=1)
    kv_out = jnp.concatenate([half_of(key_rotated_rows, True), half_of(values, True)], axis=1)
    kv_got = send(kv_out, "fsdp", swap)
    q_own = half_of(queries, False)
    q_got = send(half_of(queries, True), "fsdp", swap)
    ahead = [(i, i + behind) for i in range(count - behind)]
    far_own = send(kv_own, "seq", ahead)
    far_got = send(kv_got, "seq", ahead)
    near_own = send(jnp.where(c == 0, kv_own, far_own), "seq", cores)
    near_got = send(jnp.where(c == 0, kv_got, far_got), "seq", cores)

    starts = jnp.cumsum(doc_lengths) - doc_lengths
    base = s * (2 * rows)
    position = base + jnp.arange(2 * rows, dtype=jnp.int32)
    first = jnp.max(jnp.where(starts[None, :] <= position[:, None], starts[None, :], 0), axis=1)
    low = (jnp.maximum(first, position - (WINDOW_TOKENS - 1)) - base + WINDOW_TOKENS)[:, None]

    half = QUERY_HEADS // 2 * HEAD_SIZE
    mine = pl.pallas_call(
        functools.partial(attend_kernel, rows, heads, groups),
        out_shape=jax.ShapeDtypeStruct((2 * rows, half), jnp.bfloat16),
        in_specs=[SM, VM] + [ANY] * 8,
        out_specs=VM,
        scratch_shapes=[
            pltpu.VMEM((2 * rows, half), jnp.bfloat16),
            pltpu.VMEM((6 * rows, 2 * heads * HEAD_SIZE), jnp.bfloat16),
            pltpu.SemaphoreType.DMA((8,)),
        ],
        cost_estimate=pl.CostEstimate(flops=6_000_000_000, bytes_accessed=6_000_000, transcendentals=5_000_000),
        name="attend",
    )(flag, low, q_own, q_got, far_own, far_got, near_own, near_got, kv_own, kv_got)
    other = send(mine, "fsdp", swap)

    outer = count // 4
    if outer <= 4:
        column = [out_weight]
        for r in (1, 3, 2):
            column.append(send(out_weight, "seq", [(i, (i + 4 * r) % count) for i in range(count)]))
        shift = [0, 1, 3, 2]
        plane = column + [send(p, "seq", [(i, i ^ 2) for i in range(count)]) for p in column]
        parts = plane + [send(p, "seq", cores) for p in plane]
        at = []
        for core in range(2):
            for x in range(2):
                for r in shift:
                    at.append((((s - 4 * r) % count) ^ (2 * x)) ^ core)
        at = jnp.stack(at).astype(jnp.int32)
    else:
        parts = [lax.all_gather(out_weight, "seq", axis=0, tiled=True)]
        at = jnp.zeros((1,), jnp.int32)
    pieces = len(parts)
    width = out_weight.shape[1]
    own, peer = pl.pallas_call(
        functools.partial(project_kernel, rows, pieces),
        out_shape=(
            jax.ShapeDtypeStruct((rows, width), jnp.float32),
            jax.ShapeDtypeStruct((rows, width), jnp.bfloat16),
        ),
        in_specs=[SM, SM, VM, VM] + [ANY] * pieces,
        out_specs=(VM, VM),
        scratch_shapes=[
            pltpu.VMEM((count * out_weight.shape[0], width), jnp.bfloat16),
            pltpu.SemaphoreType.DMA((pieces,)),
        ],
        compiler_params=pltpu.CompilerParams(vmem_limit_bytes=48 * 2**20),
        cost_estimate=pl.CostEstimate(flops=6_000_000_000, bytes_accessed=20_000_000, transcendentals=0),
        name="project",
    )(flag, at, mine, other, *parts)
    got = send(peer, "fsdp", swap)

    total = residual.shape[1]
    tile = rows // 4
    block = lambda n: pl.BlockSpec((tile, n), lambda i: (i, 0))
    return pl.pallas_call(
        finish_kernel,
        grid=(rows // tile,),
        out_shape=jax.ShapeDtypeStruct(residual.shape, jnp.bfloat16),
        in_specs=[SM, block(width), block(width), block(total), pl.BlockSpec((1, total), lambda i: (0, 0))],
        out_specs=block(total),
        cost_estimate=pl.CostEstimate(flops=100_000_000, bytes_accessed=9_000_000, transcendentals=0),
        name="finish",
    )(flag, own, got, residual, norm_gain[None, :])


def solution(mesh):
    in_specs = (
        P(("seq", "fsdp"), None),
        P(("seq", "fsdp"), None),
        P(("seq", "fsdp"), None),
        P("seq", "fsdp"),
        P(("seq", "fsdp"), None),
        P(),
        P(),
    )
    out_specs = P(("seq", "fsdp"), None)
    return jax.shard_map(shards, mesh=mesh, in_specs=in_specs, out_specs=out_specs, check_vma=False)
```
